32 devices in a mesh: row: 8 (over z, core), col: 4 (over y, x).
Axes of the slice: x: 2, y: 2, z: 4, core: 2. Of those that a mesh axis runs over, the one named last changes fastest.
Arguments:
- gradient: float32 [8192, 28672], P('row', 'col'), may hold values from -100 to 100
- residual: float32 [8192, 28672], P('row', 'col'), may hold values from -3 to 3
- q_init: float32 [4, 28672], P(None, 'col'), may hold values from -5 to 5
Outputs:
- q_factor: float32 [4, 28672], P(None, 'col')
- new_residual: float32 [8192, 28672], P('row', 'col')
The draws below stay inside these ranges and needn't reach their ends.
All inputs are finite; a program needn't handle non-finite values.
Results may differ from the reference program's by a relative error of at most 0.00012.
Values sent between devices are 32-bit elements; how exact they have to be, the bound alone decides.
A program may use at most 128 MiB of HBM per device.

```python
import jax
import jax.numpy as jnp
from jax import lax

D = 8192
FF = 28672
RANK = 4
ITERS = 16


def draw_gradient(key, part):
    key_rows = jax.random.fold_in(key, 11)
    key_cols = jax.random.fold_in(key, 12)
    key_noise = jax.random.fold_in(key, 13)
    row_index = jnp.arange(D).astype(jnp.float32)
    rising = jnp.exp(jnp.log(3.0) * row_index / D)
    row_scale = rising * jnp.exp(jax.random.uniform(key_rows, (D,), jnp.float32, 0.0, jnp.log(10.0))) / 4.0
    col_scale = jnp.exp(jax.random.uniform(key_cols, (FF,), jnp.float32, 0.0, jnp.log(10.0))) / 3.0
    noise_draw = jnp.clip(jax.random.normal(key_noise, (D, FF), jnp.float32), -4.0, 4.0)
    return (noise_draw * row_scale[:, None] * col_scale[None, :]).astype(jnp.float32)


def block_scale(key, extent, shards, least, high):
    factor_of = 1.0
    for position, parts in shards:
        heights = jax.random.uniform(jax.random.fold_in(jax.random.fold_in(key, 6), position), (parts,), jnp.float32, least / len(shards), high / len(shards))
        factor_of = factor_of * jnp.repeat(jnp.exp(heights), extent[position] // parts).reshape((-1,) + (1,) * (len(extent) - 1 - position))
    return factor_of


def centred(stream_key, extent, scale, most, split=(), kind=jnp.bfloat16):
    entries = jax.random.normal(stream_key, extent, jnp.float32) * scale
    if len(split) > 0:
        entries = block_scale(stream_key, extent, split, -0.22, 0.18) * entries
    return jnp.clip(entries, min=-most, max=most).astype(kind)


def setup_inputs(seed: int = 0) -> dict:
    seeds = jax.random.split(jax.random.key(seed), 4)
    gradient = draw_gradient(jax.random.fold_in(seeds[3], 71), 0)
    residual = centred(seeds[1], (D, FF), 0.5, 3.0, ((0, 8), (1, 4)), jnp.float32)
    q_init = centred(seeds[2], (RANK, FF), 1.0, 5.0, ((1, 4),), jnp.float32)
    return dict(gradient=gradient, residual=residual, q_init=q_init)


def reference(gradient, residual, q_init):
    highest = lax.Precision.HIGHEST
    merged = gradient + residual

    def iterate(step_index, carry):
        q_current, p_previous = carry
        p_factor = lax.dot_general(q_current.astype(jnp.float32), merged.astype(jnp.float32), (((1,), (1,)), ((), ())), precision=highest, preferred_element_type=jnp.float32)
        gram = lax.dot_general(p_factor.astype(jnp.float32), p_factor.astype(jnp.float32), (((1,), (1,)), ((), ())), precision=highest, preferred_element_type=jnp.float32)
        factor_low = jnp.linalg.cholesky(gram)
        p_basis = jax.scipy.linalg.solve_triangular(factor_low, p_factor, lower=True)
        q_next = jnp.dot(p_basis.astype(jnp.float32), merged.astype(jnp.float32), precision=highest, preferred_element_type=jnp.float32)
        return (q_next, p_basis)
    start = (q_init, jnp.zeros((RANK, D), jnp.float32))
    q_factor, p_basis = lax.fori_loop(0, ITERS, iterate, start)
    approx = lax.dot_general(p_basis.astype(jnp.float32), q_factor.astype(jnp.float32), (((0,), (0,)), ((), ())), precision=highest, preferred_element_type=jnp.float32)
    return (q_factor, merged - approx)
```

```python
import functools

import jax
import jax.numpy as jnp
from jax import lax
from jax.experimental import pallas as pl
from jax.experimental.pallas import tpu as pltpu
from jax.sharding import PartitionSpec as P

ITERS = 16
MESH = pl.DeviceIdType.MESH
LANE = 128
SLOTS = 4
f32 = jnp.float32
bf16 = jnp.bfloat16


def factor(gram):
    low = [[None] * 4 for _ in range(4)]
    for i in range(4):
        for j in range(i + 1):
            rest = gram[i][j]
            for k in range(j):
                rest = rest - low[i][k] * low[j][k]
            low[i][j] = jnp.sqrt(rest) if i == j else rest / low[j][j]
    return low


def solve(low, rows):
    found = []
    for i in range(4):
        rest = rows[i]
        for k in range(i):
            rest = rest - low[i][k] * found[k]
        found.append(rest / low[i][i])
    return found


def pieces(x):
    a = x.astype(bf16).astype(f32)
    rest = x - a
    b = rest.astype(bf16).astype(f32)
    c = rest - b
    return jnp.concatenate([a, b, c, jnp.zeros_like(x)], axis=0).astype(bf16)


def fold(acc):
    return acc[0:4] + acc[4:8] + acc[8:12]


def dot(a, b):
    return jnp.dot(a, b, preferred_element_type=f32)


def kernel(
    n_row, n_col, width, load_cols,
    grad_ref, res_ref, q0_ref, q_out, p_out,
    hi, lo, hi_t, lo_t, g_slot, r_slot,
    ps, p_acc, p_in, p_now, c_in, c_sum, g_in, low_b,
    g_sem, r_sem, p_send, p_recv, c_send, c_recv, s_send, s_recv, m_send, m_recv,
):
    rows, cols = hi.shape
    n = cols // width
    me_row, me_col = lax.axis_index("row"), lax.axis_index("col")
    col_peer = lambda d: (me_row, lax.rem(me_col + d, n_col))
    row_peer = lambda d: (lax.rem(me_row + d, n_row), me_col)
    mid = n_row // 4
    own = [max(2 * mid - 1, 0), min(2 * mid + 1, n_row - 1)]

    barrier = pltpu.get_barrier_semaphore()
    for d in range(1, n_col):
        pl.semaphore_signal(barrier, inc=1, device_id=col_peer(d), device_id_type=MESH)
    for d in range(1, n_row):
        pl.semaphore_signal(barrier, inc=1, device_id=row_peer(d), device_id_type=MESH)

    across = cols // load_cols
    blocks = (rows // LANE) * across

    def load(b):
        s = lax.rem(b, SLOTS)
        part = (
            pl.ds(pl.multiple_of((b // across) * LANE, LANE), LANE),
            pl.ds(pl.multiple_of(lax.rem(b, across) * load_cols, LANE), load_cols),
        )
        return (
            pltpu.make_async_copy(grad_ref.at[part], g_slot.at[s], g_sem.at[s]),
            pltpu.make_async_copy(res_ref.at[part], r_slot.at[s], r_sem.at[s]),
        )

    for b in range(SLOTS):
        for copy in load(b):
            copy.start()
    c_sum_rows = q0_ref[...]
    for k in range(n):
        c_sum[k] = c_sum_rows[:, k * width : (k + 1) * width]
    for i in range(4):
        for j in range(4):
            low_b[4 * i + j] = jnp.full((1, rows), 1.0 if i == j else 0.0, f32)

    @pl.loop(0, blocks)
    def _(b):
        for copy in load(b):
            copy.wait()
        s = lax.rem(b, SLOTS)
        at_row = pl.ds(pl.multiple_of((b // across) * LANE, LANE), LANE)
        at_col = pl.multiple_of(lax.rem(b, across) * load_cols, LANE)
        for t in range(load_cols // LANE):
            part = slice(t * LANE, (t + 1) * LANE)
            x = g_slot[s, :, part] + r_slot[s, :, part]
            top = x.astype(bf16)
            low = (x - top.astype(f32)).astype(bf16)
            here = pl.ds(pl.multiple_of(at_col + t * LANE, LANE), LANE)
            hi[at_row, here] = top
            lo[at_row, here] = low
            hi_t[here, at_row] = top.T
            lo_t[here, at_row] = low.T

        @pl.when(b + SLOTS < blocks)
        def _():
            for copy in load(b + SLOTS):
                copy.start()

    pl.semaphore_wait(barrier, n_col + n_row - 2)

    def to_owner(k):
        mine = c_in.at[me_row, k]
        return pltpu.make_async_remote_copy(
            src_ref=mine, dst_ref=mine, send_sem=c_send.at[k], recv_sem=c_recv.at[me_row, k],
            device_id=(own[k % 2], me_col), device_id_type=MESH,
        )

    def from_source(k, d):
        src = lax.rem(me_row + d, n_row)
        theirs = c_in.at[src, k]
        return pltpu.make_async_remote_copy(
            src_ref=theirs, dst_ref=theirs, send_sem=c_send.at[k], recv_sem=c_recv.at[src, k],
            device_id=row_peer(d), device_id_type=MESH,
        )

    def spread(k, d):
        return pltpu.make_async_remote_copy(
            src_ref=c_sum.at[k], dst_ref=c_sum.at[k], send_sem=s_send.at[k, d], recv_sem=s_recv.at[k],
            device_id=row_peer(d), device_id_type=MESH,
        )

    def gram_copy(par, d):
        mine = g_in.at[par, me_row]
        return pltpu.make_async_remote_copy(
            src_ref=mine, dst_ref=mine, send_sem=m_send.at[d], recv_sem=m_recv.at[par, d],
            device_id=row_peer(d), device_id_type=MESH,
        )

    def p_copy(par, d):
        mine = p_in.at[par, me_col]
        return pltpu.make_async_remote_copy(
            src_ref=mine, dst_ref=mine, send_sem=p_send.at[d], recv_sem=p_recv.at[par, d],
            device_id=col_peer(d), device_id_type=MESH,
        )

    is_own = [me_row == own[0], me_row == own[1]]

    def place(i):
        first = list(range(0, n, 2)) + list(range(1, n, 2))
        second = list(range(1, n, 2)) + list(range(0, n, 2))
        return jnp.where(is_own[0], first[i], jnp.where(is_own[1], second[i], i))

    def owned(k):
        even = lax.rem(k, 2) == 0
        return jnp.logical_or(
            jnp.logical_and(even, is_own[0]), jnp.logical_and(jnp.logical_not(even), is_own[1])
        )

    def settle(k):
        @pl.when(owned(k))
        def _():
            for d in range(1, n_row):
                from_source(k, d).wait_recv()
            total = c_in[0, k]
            for s in range(1, n_row):
                total = total + c_in[s, k]
            c_sum[k] = total
            for d in range(1, n_row):
                spread(k, d).start()

        @pl.when(jnp.logical_not(owned(k)))
        def _():
            spread(k, 1).wait_recv()

    def finish_sends():
        for k in range(n):
            @pl.when(is_own[k % 2])
            def _():
                for d in range(1, n_row):
                    spread(k, d).wait_send()

            @pl.when(jnp.logical_not(is_own[k % 2]))
            def _():
                to_owner(k).wait_send()

    def find_low(par):
        for d in range(1, n_row):
            gram_copy(par, d).wait()
        total = g_in[par, 0]
        for s in range(1, n_row):
            total = total + g_in[par, s]
        gram = [[total[i : i + 1, j : j + 1] for j in range(4)] for i in range(4)]
        low = factor(gram)
        for i in range(4):
            for j in range(i + 1):
                low_b[4 * i + j] = jnp.broadcast_to(low[i][j], (1, rows))

    def low_of(lanes):
        return [[low_b[4 * i + j, :, :lanes] for j in range(i + 1)] for i in range(4)]

    def iterate(step, carry):
        par = lax.rem(step, 2)
        p_acc[...] = jnp.zeros_like(p_acc)
        for i in range(n):
            k = place(i)

            @pl.when(step > 0)
            def _():
                settle(k)

            q_now = pieces(c_sum[k])
            here = pl.ds(pl.multiple_of(k * width, width), width)
            p_acc[...] += dot(q_now, hi_t[here, :]) + dot(q_now, lo_t[here, :])
            if i == min(1, n - 1):

                @pl.when(step > 0)
                def _():
                    find_low(lax.rem(step + 1, 2))

        p_in[par, me_col] = fold(p_acc[...])
        for d in range(1, n_col):
            p_copy(par, d).start()

        @pl.when(step > 0)
        def _():
            finish_sends()

        for d in range(1, n_col):
            p_copy(par, d).wait()
        total = p_in[par, 0]
        for c in range(1, n_col):
            total = total + p_in[par, c]
        p_rows = solve(low_of(rows), [total[r : r + 1] for r in range(4)])
        p_new = jnp.concatenate(p_rows, axis=0)
        p_now[...] = p_new
        ps[...] = pieces(p_new)

        lane_id = lax.broadcasted_iota(jnp.int32, (4, LANE), 1)
        corner = jnp.zeros((4, LANE), f32)
        for i in range(4):
            dots = jnp.sum(p_new * p_new[i : i + 1], axis=1, keepdims=True)
            corner = jnp.where(lane_id == i, dots, corner)
        g_in[par, me_row] = corner

        for k in range(n):
            part = slice(k * width, (k + 1) * width)
            acc = dot(ps[...], hi[:, part]) + dot(ps[...], lo[:, part])
            c_in[me_row, k] = fold(acc)

            @pl.when(jnp.logical_not(is_own[k % 2]))
            def _():
                to_owner(k).start()

            if k == 0:
                for d in range(1, n_row):
                    gram_copy(par, d).start()
        return carry

    lax.fori_loop(0, ITERS, iterate, 0)
    for i in range(n):
        settle(place(i))
    find_low((ITERS - 1) % 2)
    finish_sends()
    p_rows = solve(low_of(rows), [p_now[r : r + 1] for r in range(4)])
    p_out[...] = jnp.concatenate(p_rows, axis=0)
    low = [[low_b[4 * i + j, :, :1] for j in range(i + 1)] for i in range(4)]
    for k in range(n):
        q_rows = solve(low, [c_sum[k, r : r + 1] for r in range(4)])
        q_out[:, k * width : (k + 1) * width] = jnp.concatenate(q_rows, axis=0)


def best_width(cols, most):
    return max(w for w in range(LANE, most + 1, LANE) if cols % w == 0)


def shards(n_row, n_col, gradient, residual, q_init):
    rows, cols = gradient.shape
    width = best_width(cols, max(LANE, cols // 7))
    load_cols = best_width(cols, 1024)
    n = cols // width
    vmem = lambda *shape: pltpu.VMEM(shape, f32)
    half = lambda *shape: pltpu.VMEM(shape, bf16)
    dma = pltpu.SemaphoreType.DMA
    q_factor, p_basis = pl.pallas_call(
        functools.partial(kernel, n_row, n_col, width, load_cols),
        out_shape=(
            jax.ShapeDtypeStruct((4, cols), f32),
            jax.ShapeDtypeStruct((4, rows), f32),
        ),
        in_specs=[
            pl.BlockSpec(memory_space=pl.ANY),
            pl.BlockSpec(memory_space=pl.ANY),
            pl.BlockSpec(memory_space=pltpu.VMEM),
        ],
        out_specs=(
            pl.BlockSpec(memory_space=pltpu.VMEM),
            pl.BlockSpec(memory_space=pltpu.VMEM),
        ),
        scratch_shapes=[
            half(rows, cols),
            half(rows, cols),
            half(cols, rows),
            half(cols, rows),
            vmem(SLOTS, LANE, load_cols),
            vmem(SLOTS, LANE, load_cols),
            half(16, rows),
            vmem(16, rows),
            vmem(2, n_col, 4, rows),
            vmem(4, rows),
            vmem(n_row, n, 4, width),
            vmem(n, 4, width),
            vmem(2, n_row, 4, LANE),
            vmem(16, 1, rows),
            dma((SLOTS,)),
            dma((SLOTS,)),
            dma((n_col,)),
            dma((2, n_col)),
            dma((n,)),
            dma((n_row, n)),
            dma((n, n_row)),
            dma((n,)),
            dma((n_row,)),
            dma((2, n_row)),
        ],
        compiler_params=pltpu.CompilerParams(
            collective_id=0, has_side_effects=True, vmem_limit_bytes=67043328
        ),
    )(gradient, residual, q_init)
    left = gradient + residual
    for r in range(4):
        left = left - p_basis[r][:, None] * q_factor[r][None, :]
    return (q_factor, left)


def solution(mesh):
    in_specs = (P("row", "col"), P("row", "col"), P(None, "col"))
    out_specs = (P(None, "col"), P("row", "col"))
    body = functools.partial(shards, mesh.shape["row"], mesh.shape["col"])
    return jax.shard_map(body, mesh=mesh, in_specs=in_specs, out_specs=out_specs, check_vma=False)
```

```python
import functools

import jax
import jax.numpy as jnp
from jax import lax
from jax.experimental import pallas as pl
from jax.experimental.pallas import tpu as pltpu
from jax.sharding import PartitionSpec as P

ITERS = 16
MESH = pl.DeviceIdType.MESH
LANE = 128
SLOTS = 5
GROUP = 2 * LANE
f32 = jnp.float32
bf16 = jnp.bfloat16


def factor(gram):
    low = [[None] * 4 for _ in range(4)]
    for i in range(4):
        for j in range(i + 1):
            rest = gram[i][j]
            for k in range(j):
                rest = rest - low[i][k] * low[j][k]
            low[i][j] = jnp.sqrt(rest) if i == j else rest / low[j][j]
    return low


def solve(low, rows):
    found = []
    for i in range(4):
        rest = rows[i]
        for k in range(i):
            rest = rest - low[i][k] * found[k]
        found.append(rest / low[i][i])
    return found


def split(x):
    a = x.astype(bf16).astype(f32)
    rest = x - a
    b = rest.astype(bf16).astype(f32)
    return a, b, rest - b


def pieces(x):
    return jnp.concatenate([*split(x), jnp.zeros_like(x)], axis=0).astype(bf16)


def fold(acc):
    return acc[0:4] + acc[4:8] + acc[8:12]


def dot(a, b):
    return jnp.dot(a, b, preferred_element_type=f32)


def kernel(
    n_row, n_col, parts, load_cols,
    grad_ref, res_ref, q0_ref, q_out, hi, lo, left_out, right_out,
    hi_t, lo_t, g_slot, r_slot,
    qs, ps, p_acc, p_in, p_now, c_in, c_sum, g_in, low_b,
    g_sem, r_sem, p_send, p_recv, c_send, c_recv, s_send, s_recv, m_send, m_recv,
):
    rows, cols = hi.shape
    n = len(parts)
    me_row, me_col = lax.axis_index("row"), lax.axis_index("col")
    row_peer = lambda d: (lax.rem(me_row + d, n_row), me_col)
    if n_col & (n_col - 1) == 0:
        col_peer = lambda d: (me_row, me_col ^ d)
    else:
        col_peer = lambda d: (me_row, lax.rem(me_col + d, n_col))
    col_order = list(range(n_col - 1, 0, -1))
    mid = n_row // 4
    own = [max(2 * mid - 1, 0), min(2 * mid + 1, n_row - 1)]
    is_own = [me_row == own[0], me_row == own[1]]

    barrier = pltpu.get_barrier_semaphore()
    for d in range(1, n_col):
        pl.semaphore_signal(barrier, inc=1, device_id=col_peer(d), device_id_type=MESH)
    for d in range(1, n_row):
        pl.semaphore_signal(barrier, inc=1, device_id=row_peer(d), device_id_type=MESH)

    across = cols // load_cols
    blocks = (rows // LANE) * across
    group = GROUP if rows % GROUP == 0 else LANE
    per_group = (group // LANE) * across

    def load(b):
        s = lax.rem(b, SLOTS)
        part = (
            pl.ds(pl.multiple_of((b // across) * LANE, LANE), LANE),
            pl.ds(pl.multiple_of(lax.rem(b, across) * load_cols, LANE), load_cols),
        )
        return (
            pltpu.make_async_copy(grad_ref.at[part], g_slot.at[s], g_sem.at[s]),
            pltpu.make_async_copy(res_ref.at[part], r_slot.at[s], r_sem.at[s]),
        )

    for b in range(SLOTS):
        for copy in load(b):
            copy.start()
    qs[...] = pieces(q0_ref[...])
    for i in range(4):
        for j in range(4):
            low_b[4 * i + j] = jnp.full((1, rows), 1.0 if i == j else 0.0, f32)

    @pl.loop(0, rows // group)
    def _(r):
        @pl.loop(0, per_group)
        def _(u):
            b = r * per_group + u
            for copy in load(b):
                copy.wait()
            s = lax.rem(b, SLOTS)
            at_row = pl.ds(pl.multiple_of((b // across) * LANE, LANE), LANE)
            at_col = pl.multiple_of(lax.rem(b, across) * load_cols, LANE)
            for t in range(load_cols // LANE):
                part = slice(t * LANE, (t + 1) * LANE)
                x = g_slot[s, :, part] + r_slot[s, :, part]
                top = x.astype(bf16)
                low = (x - top.astype(f32)).astype(bf16)
                here = pl.ds(pl.multiple_of(at_col + t * LANE, LANE), LANE)
                hi[at_row, here] = top
                lo[at_row, here] = low
                hi_t[here, at_row] = top.T
                lo_t[here, at_row] = low.T

            @pl.when(b + SLOTS < blocks)
            def _():
                for copy in load(b + SLOTS):
                    copy.start()

        here = pl.ds(pl.multiple_of(r * group, LANE), group)
        p_acc[:, here] = dot(qs[...], hi_t[:, here]) + dot(qs[...], lo_t[:, here])

    pl.semaphore_wait(barrier, n_col + n_row - 2)

    def to_owner(k):
        mine = c_in.at[me_row, :, parts[k]]
        return pltpu.make_async_remote_copy(
            src_ref=mine, dst_ref=mine, send_sem=c_send.at[k], recv_sem=c_recv.at[me_row, k],
            device_id=(own[k % 2], me_col), device_id_type=MESH,
        )

    def from_source(k, src):
        theirs = c_in.at[src, :, parts[k]]
        return pltpu.make_async_remote_copy(
            src_ref=theirs, dst_ref=theirs, send_sem=c_send.at[k], recv_sem=c_recv.at[src, k],
            device_id=(src, me_col), device_id_type=MESH,
        )

    def spread(k, dest):
        whole = c_sum.at[:, parts[k]]
        return pltpu.make_async_remote_copy(
            src_ref=whole, dst_ref=whole, send_sem=s_send.at[k, dest], recv_sem=s_recv.at[k],
            device_id=(dest, me_col), device_id_type=MESH,
        )

    def gram_copy(par, d):
        mine = g_in.at[par, me_row]
        return pltpu.make_async_remote_copy(
            src_ref=mine, dst_ref=mine, send_sem=m_send.at[d], recv_sem=m_recv.at[par, d],
            device_id=row_peer(d), device_id_type=MESH,
        )

    def p_copy(par, d):
        mine = p_in.at[par, me_col]
        return pltpu.make_async_remote_copy(
            src_ref=mine, dst_ref=mine, send_sem=p_send.at[d], recv_sem=p_recv.at[par, d],
            device_id=col_peer(d), device_id_type=MESH,
        )

    def far_first(o):
        others = [s for s in range(n_row) if s != o]
        return sorted(others, key=lambda s: (-abs(s // 2 - o // 2), s % 2))

    def settle():
        for side in range(2):
            @pl.when(is_own[side])
            def _():
                others = far_first(own[side])
                for k in range(side, n, 2):
                    for src in reversed(others):
                        from_source(k, src).wait_recv()
                    total = c_in[0, :, parts[k]]
                    for s in range(1, n_row):
                        total = total + c_in[s, :, parts[k]]
                    c_sum[:, parts[k]] = total
                    for dest in others:
                        spread(k, dest).start()

    def arrive(k):
        @pl.when(jnp.logical_not(is_own[k % 2]))
        def _():
            spread(k, own[k % 2]).wait_recv()

    def finish_sends():
        for side in range(2):
            @pl.when(is_own[side])
            def _():
                for k in range(side, n, 2):
                    for dest in far_first(own[side]):
                        spread(k, dest).wait_send()

            @pl.when(jnp.logical_not(is_own[side]))
            def _():
                for k in range(side, n, 2):
                    to_owner(k).wait_send()

    def find_low(par):
        for d in range(1, n_row):
            gram_copy(par, d).wait()
        total = g_in[par, 0]
        for s in range(1, n_row):
            total = total + g_in[par, s]
        gram = [[total[i : i + 1, j : j + 1] for j in range(4)] for i in range(4)]
        low = factor(gram)
        for i in range(4):
            for j in range(i + 1):
                low_b[4 * i + j] = jnp.broadcast_to(low[i][j], (1, rows))

    def low_of(lanes):
        return [[low_b[4 * i + j, :, :lanes] for j in range(i + 1)] for i in range(4)]

    def iterate(step, carry):
        par = lax.rem(step, 2)

        @pl.when(step > 0)
        def _():
            settle()
            find_low(lax.rem(step + 1, 2))
            for k in range(n):
                arrive(k)
                q_now = pieces(c_sum[:, parts[k]])
                more = dot(q_now, hi_t[parts[k], :]) + dot(q_now, lo_t[parts[k], :])
                p_acc[...] = more if k == 0 else p_acc[...] + more

        p_in[par, me_col] = fold(p_acc[...])
        for d in col_order:
            p_copy(par, d).start()

        @pl.when(step > 0)
        def _():
            finish_sends()

        for d in reversed(col_order):
            p_copy(par, d).wait()
        total = p_in[par, 0]
        for c in range(1, n_col):
            total = total + p_in[par, c]
        p_rows = solve(low_of(rows), [total[r : r + 1] for r in range(4)])
        p_new = jnp.concatenate(p_rows, axis=0)
        p_now[...] = p_new
        ps[...] = pieces(p_new)

        lane_id = lax.broadcasted_iota(jnp.int32, (4, LANE), 1)
        corner = jnp.zeros((4, LANE), f32)
        for i in range(4):
            dots = jnp.sum(p_new * p_new[i : i + 1], axis=1, keepdims=True)
            corner = jnp.where(lane_id == i, dots, corner)
        g_in[par, me_row] = corner

        for k in range(n):
            acc = dot(ps[...], hi[:, parts[k]]) + dot(ps[...], lo[:, parts[k]])
            c_in[me_row, :, parts[k]] = fold(acc)

            @pl.when(jnp.logical_not(is_own[k % 2]))
            def _():
                to_owner(k).start()

            if k == 0:
                for d in range(1, n_row):
                    gram_copy(par, d).start()
        return carry

    lax.fori_loop(0, ITERS, iterate, 0)
    settle()
    find_low((ITERS - 1) % 2)
    p_rows = solve(low_of(rows), [p_now[r : r + 1] for r in range(4)])
    a, b, c = split(jnp.concatenate(p_rows, axis=0))
    zero = jnp.zeros_like(a)
    stacked = jnp.concatenate([a, a, b, b, a, c, zero, zero], axis=0)
    for t in range(rows // LANE):
        part = slice(t * LANE, (t + 1) * LANE)
        left_out[part, :] = stacked[:, part].T.astype(bf16)
    low = [[low_b[4 * i + j, :, :1] for j in range(i + 1)] for i in range(4)]
    for k in range(n):
        arrive(k)
        q_rows = solve(low, [c_sum[r : r + 1, parts[k]] for r in range(4)])
        q_new = jnp.concatenate(q_rows, axis=0)
        q_out[:, parts[k]] = q_new
        a, b, c = split(q_new)
        zero = jnp.zeros_like(a)
        right_out[:, parts[k]] = jnp.concatenate([a, b, a, b, c, a, zero, zero], axis=0).astype(bf16)
    finish_sends()


def subtract(load_cols, hi, lo, left, right, out_ref, slot, sem):
    rows, cols = hi.shape
    across = cols // load_cols
    blocks = (rows // LANE) * across

    def store(b):
        s = lax.rem(b, SLOTS)
        part = (
            pl.ds(pl.multiple_of((b // across) * LANE, LANE), LANE),
            pl.ds(pl.multiple_of(lax.rem(b, across) * load_cols, LANE), load_cols),
        )
        return pltpu.make_async_copy(slot.at[s], out_ref.at[part], sem.at[s])

    @pl.loop(0, blocks)
    def _(b):
        @pl.when(b >= SLOTS)
        def _():
            store(b - SLOTS).wait()

        at_row = pl.ds(pl.multiple_of((b // across) * LANE, LANE), LANE)
        at_col = pl.ds(pl.multiple_of(lax.rem(b, across) * load_cols, LANE), load_cols)
        product = dot(left[at_row, :], right[:, at_col])
        x = hi[at_row, at_col].astype(f32) + lo[at_row, at_col].astype(f32)
        slot[lax.rem(b, SLOTS)] = x - product
        store(b).start()

    for b in range(max(blocks - SLOTS, 0), blocks):
        store(b).wait()


def best_width(cols, most):
    return max(w for w in range(LANE, most + 1, LANE) if cols % w == 0)


def chunks(cols):
    width = best_width(cols, max(LANE, cols // 7))
    sizes = [width] * (cols // width)
    if width % (2 * LANE) == 0:
        sizes[-1:] = [width // 2] * 2
    ends = [sum(sizes[: k + 1]) for k in range(len(sizes))]
    return [slice(end - size, end) for end, size in zip(ends, sizes)]


def shards(n_row, n_col, gradient, residual, q_init):
    rows, cols = gradient.shape
    parts = chunks(cols)
    load_cols = best_width(cols, 1024)
    n = len(parts)
    vmem = lambda *shape: pltpu.VMEM(shape, f32)
    half = lambda *shape: pltpu.VMEM(shape, bf16)
    dma = pltpu.SemaphoreType.DMA
    anywhere = pl.BlockSpec(memory_space=pl.ANY)
    held = pl.BlockSpec(memory_space=pltpu.VMEM)
    q_factor, hi, lo, left, right = pl.pallas_call(
        functools.partial(kernel, n_row, n_col, parts, load_cols),
        out_shape=(
            jax.ShapeDtypeStruct((4, cols), f32),
            half(rows, cols),
            half(rows, cols),
            half(rows, 32),
            half(32, cols),
        ),
        in_specs=[anywhere, anywhere, held],
        out_specs=(held,) * 5,
        scratch_shapes=[
            half(cols, rows),
            half(cols, rows),
            vmem(SLOTS, LANE, load_cols),
            vmem(SLOTS, LANE, load_cols),
            half(16, cols),
            half(16, rows),
            vmem(16, rows),
            vmem(2, n_col, 4, rows),
            vmem(4, rows),
            vmem(n_row, 4, cols),
            vmem(4, cols),
            vmem(2, n_row, 4, LANE),
            vmem(16, 1, rows),
            dma((SLOTS,)),
            dma((SLOTS,)),
            dma((n_col,)),
            dma((2, n_col)),
            dma((n,)),
            dma((n_row, n)),
            dma((n, n_row)),
            dma((n,)),
            dma((n_row,)),
            dma((2, n_row)),
        ],
        compiler_params=pltpu.CompilerParams(
            collective_id=0, has_side_effects=True, vmem_limit_bytes=35 * 1024 * 1024
        ),
    )(gradient, residual, q_init)
    new_residual = pl.pallas_call(
        functools.partial(subtract, load_cols),
        out_shape=jax.ShapeDtypeStruct((rows, cols), f32),
        in_specs=[held] * 4,
        out_specs=anywhere,
        scratch_shapes=[vmem(SLOTS, LANE, load_cols), dma((SLOTS,))],
        compiler_params=pltpu.CompilerParams(vmem_limit_bytes=4 * 1024 * 1024),
    )(hi, lo, left, right)
    return (q_factor, new_residual)


def solution(mesh):
    in_specs = (P("row", "col"), P("row", "col"), P(None, "col"))
    out_specs = (P(None, "col"), P("row", "col"))
    body = functools.partial(shards, mesh.shape["row"], mesh.shape["col"])
    return jax.shard_map(body, mesh=mesh, in_specs=in_specs, out_specs=out_specs, check_vma=False)
```

```python
import functools

import jax
import jax.numpy as jnp
from jax import lax
from jax.experimental import pallas as pl
from jax.experimental.pallas import tpu as pltpu
from jax.sharding import PartitionSpec as P

ITERS = 16
MESH = pl.DeviceIdType.MESH
LANE = 128
SLOTS = 5
GROUP = 2 * LANE
STRIP = 4 * LANE
f32 = jnp.float32
bf16 = jnp.bfloat16


def factor(gram):
    low = [[None] * 4 for _ in range(4)]
    for i in range(4):
        for j in range(i + 1):
            rest = gram[i][j]
            for k in range(j):
                rest = rest - low[i][k] * low[j][k]
            low[i][j] = jnp.sqrt(rest) if i == j else rest / low[j][j]
    return low


def solve(low, rows):
    found = []
    for i in range(4):
        rest = rows[i]
        for k in range(i):
            rest = rest - low[i][k] * found[k]
        found.append(rest / low[i][i])
    return found


def split(x):
    a = x.astype(bf16).astype(f32)
    rest = x - a
    b = rest.astype(bf16).astype(f32)
    return a, b, rest - b


def pieces(x):
    return jnp.concatenate([*split(x), jnp.zeros_like(x)], axis=0).astype(bf16)


def fold(acc):
    return acc[0:4] + acc[4:8] + acc[8:12]


def dot(a, b):
    return jnp.dot(a, b, preferred_element_type=f32)


def kernel(
    n_row, n_col, parts, load_cols,
    grad_ref, res_ref, q0_ref, q_out, hi, lo, left_out, right_out,
    hi_t, lo_t, g_slot, r_slot,
    qs, ps, p_acc, p_in, p_now, c_in, c_sum, g_in, low_b,
    g_sem, r_sem, p_send, p_recv, c_send, c_recv, s_send, s_recv, m_send, m_recv,
):
    rows, cols = hi.shape
    n = len(parts)
    me_row, me_col = lax.axis_index("row"), lax.axis_index("col")
    row_peer = lambda d: (lax.rem(me_row + d, n_row), me_col)
    if n_col & (n_col - 1) == 0:
        col_peer = lambda d: (me_row, me_col ^ d)
    else:
        col_peer = lambda d: (me_row, lax.rem(me_col + d, n_col))
    col_order = list(range(n_col - 1, 0, -1))
    mid = n_row // 4
    own = [max(2 * mid - 1, 0), min(2 * mid + 1, n_row - 1)]
    is_own = [me_row == own[0], me_row == own[1]]

    barrier = pltpu.get_barrier_semaphore()
    for d in range(1, n_col):
        pl.semaphore_signal(barrier, inc=1, device_id=col_peer(d), device_id_type=MESH)
    for d in range(1, n_row):
        pl.semaphore_signal(barrier, inc=1, device_id=row_peer(d), device_id_type=MESH)

    across = cols // load_cols
    blocks = (rows // LANE) * across
    group = GROUP if rows % GROUP == 0 else LANE
    per_group = (group // LANE) * across
    share = cols // per_group

    def load(b):
        s = lax.rem(b, SLOTS)
        part = (
            pl.ds(pl.multiple_of((b // across) * LANE, LANE), LANE),
            pl.ds(pl.multiple_of(lax.rem(b, across) * load_cols, LANE), load_cols),
        )
        return (
            pltpu.make_async_copy(grad_ref.at[part], g_slot.at[s], g_sem.at[s]),
            pltpu.make_async_copy(res_ref.at[part], r_slot.at[s], r_sem.at[s]),
        )

    for b in range(SLOTS):
        for copy in load(b):
            copy.start()
    qs[...] = pieces(q0_ref[...])
    for i in range(4):
        for j in range(4):
            low_b[4 * i + j] = jnp.full((1, rows), 1.0 if i == j else 0.0, f32)

    @pl.loop(0, rows // group)
    def _(r):
        @pl.loop(0, per_group)
        def _(u):
            b = r * per_group + u
            for copy in load(b):
                copy.wait()
            s = lax.rem(b, SLOTS)
            at_row = pl.ds(pl.multiple_of((b // across) * LANE, LANE), LANE)
            at_col = pl.multiple_of(lax.rem(b, across) * load_cols, LANE)
            before = pl.ds(pl.multiple_of(jnp.maximum(r - 1, 0) * group, LANE), group)
            deep = pl.ds(pl.multiple_of(u * share, LANE), share)
            more = dot(qs[:, deep], hi_t[deep, before]) + dot(qs[:, deep], lo_t[deep, before])
            p_acc[:, before] = more + jnp.where(u == 0, 0.0, p_acc[:, before])
            for t in range(load_cols // LANE):
                part = slice(t * LANE, (t + 1) * LANE)
                x = g_slot[s, :, part] + r_slot[s, :, part]
                top = x.astype(bf16)
                low = (x - top.astype(f32)).astype(bf16)
                here = pl.ds(pl.multiple_of(at_col + t * LANE, LANE), LANE)
                hi[at_row, here] = top
                lo[at_row, here] = low
                hi_t[here, at_row] = top.T
                lo_t[here, at_row] = low.T

            @pl.when(b + SLOTS < blocks)
            def _():
                for copy in load(b + SLOTS):
                    copy.start()


    last = slice(rows - group, rows)
    p_acc[:, last] = dot(qs[...], hi_t[:, last]) + dot(qs[...], lo_t[:, last])
    pl.semaphore_wait(barrier, n_col + n_row - 2)

    def to_owner(k):
        mine = c_in.at[me_row, :, parts[k]]
        return pltpu.make_async_remote_copy(
            src_ref=mine, dst_ref=mine, send_sem=c_send.at[k], recv_sem=c_recv.at[me_row, k],
            device_id=(own[k % 2], me_col), device_id_type=MESH,
        )

    def from_source(k, src):
        theirs = c_in.at[src, :, parts[k]]
        return pltpu.make_async_remote_copy(
            src_ref=theirs, dst_ref=theirs, send_sem=c_send.at[k], recv_sem=c_recv.at[src, k],
            device_id=(src, me_col), device_id_type=MESH,
        )

    def spread(k, dest):
        whole = c_sum.at[:, parts[k]]
        return pltpu.make_async_remote_copy(
            src_ref=whole, dst_ref=whole, send_sem=s_send.at[k, dest], recv_sem=s_recv.at[k],
            device_id=(dest, me_col), device_id_type=MESH,
        )

    def gram_copy(par, d):
        mine = g_in.at[par, me_row]
        return pltpu.make_async_remote_copy(
            src_ref=mine, dst_ref=mine, send_sem=m_send.at[d], recv_sem=m_recv.at[par, d],
            device_id=row_peer(d), device_id_type=MESH,
        )

    def p_copy(par, d):
        mine = p_in.at[par, me_col]
        return pltpu.make_async_remote_copy(
            src_ref=mine, dst_ref=mine, send_sem=p_send.at[d], recv_sem=p_recv.at[par, d],
            device_id=col_peer(d), device_id_type=MESH,
        )

    def far_first(o):
        others = [s for s in range(n_row) if s != o]
        return sorted(others, key=lambda s: (-abs(s // 2 - o // 2), s % 2))

    def settle():
        for side in range(2):
            @pl.when(is_own[side])
            def _():
                others = far_first(own[side])
                for k in range(side, n, 2):
                    for src in reversed(others):
                        from_source(k, src).wait_recv()
                    total = c_in[0, :, parts[k]]
                    for s in range(1, n_row):
                        total = total + c_in[s, :, parts[k]]
                    c_sum[:, parts[k]] = total
                    for dest in others:
                        spread(k, dest).start()

    def arrive(k):
        @pl.when(jnp.logical_not(is_own[k % 2]))
        def _():
            spread(k, own[k % 2]).wait_recv()

    def finish_sends():
        for side in range(2):
            @pl.when(is_own[side])
            def _():
                for k in range(side, n, 2):
                    for dest in far_first(own[side]):
                        spread(k, dest).wait_send()

            @pl.when(jnp.logical_not(is_own[side]))
            def _():
                for k in range(side, n, 2):
                    to_owner(k).wait_send()

    def find_low(par):
        for d in range(1, n_row):
            gram_copy(par, d).wait()
        total = g_in[par, 0]
        for s in range(1, n_row):
            total = total + g_in[par, s]
        gram = [[total[i : i + 1, j : j + 1] for j in range(4)] for i in range(4)]
        low = factor(gram)
        for i in range(4):
            for j in range(i + 1):
                low_b[4 * i + j] = jnp.broadcast_to(low[i][j], (1, rows))

    def low_of(lanes):
        return [[low_b[4 * i + j, :, :lanes] for j in range(i + 1)] for i in range(4)]

    def iterate(step, carry):
        par = lax.rem(step, 2)

        @pl.when(step > 0)
        def _():
            settle()
            find_low(lax.rem(step + 1, 2))
            for k in range(n):
                arrive(k)
                q_now = pieces(c_sum[:, parts[k]])
                more = dot(q_now, hi_t[parts[k], :]) + dot(q_now, lo_t[parts[k], :])
                p_acc[...] = more if k == 0 else p_acc[...] + more

        p_in[par, me_col] = fold(p_acc[...])
        for d in col_order:
            p_copy(par, d).start()

        @pl.when(step > 0)
        def _():
            finish_sends()

        for d in reversed(col_order):
            p_copy(par, d).wait()
        total = p_in[par, 0]
        for c in range(1, n_col):
            total = total + p_in[par, c]
        p_rows = solve(low_of(rows), [total[r : r + 1] for r in range(4)])
        p_new = jnp.concatenate(p_rows, axis=0)
        p_now[...] = p_new
        ps[...] = pieces(p_new)

        lane_id = lax.broadcasted_iota(jnp.int32, (4, LANE), 1)
        corner = jnp.zeros((4, LANE), f32)
        for i in range(4):
            dots = jnp.sum(p_new * p_new[i : i + 1], axis=1, keepdims=True)
            corner = jnp.where(lane_id == i, dots, corner)
        g_in[par, me_row] = corner

        for k in range(n):
            acc = dot(ps[...], hi[:, parts[k]]) + dot(ps[...], lo[:, parts[k]])
            c_in[me_row, :, parts[k]] = fold(acc)

            @pl.when(jnp.logical_not(is_own[k % 2]))
            def _():
                to_owner(k).start()

            if k == 0:
                for d in range(1, n_row):
                    gram_copy(par, d).start()
        return carry

    lax.fori_loop(0, ITERS, iterate, 0)
    settle()
    find_low((ITERS - 1) % 2)
    p_rows = solve(low_of(rows), [p_now[r : r + 1] for r in range(4)])
    a, b, c = split(jnp.concatenate(p_rows, axis=0))
    zero = jnp.zeros_like(a)
    stacked = jnp.concatenate([a, a, b, b, a, c, zero, zero], axis=0)
    for t in range(rows // LANE):
        part = slice(t * LANE, (t + 1) * LANE)
        left_out[part, :] = stacked[:, part].T.astype(bf16)
    low = [[low_b[4 * i + j, :, :1] for j in range(i + 1)] for i in range(4)]
    for k in range(n):
        arrive(k)
        q_rows = solve(low, [c_sum[r : r + 1, parts[k]] for r in range(4)])
        q_new = jnp.concatenate(q_rows, axis=0)
        q_out[:, parts[k]] = q_new
        a, b, c = split(q_new)
        zero = jnp.zeros_like(a)
        right_out[:, parts[k]] = jnp.concatenate([a, b, a, b, c, a, zero, zero], axis=0).astype(bf16)
    finish_sends()


def subtract(load_cols, hi, lo, left, right, out_ref, slot, sem):
    rows, cols = hi.shape
    across = cols // load_cols
    blocks = (rows // LANE) * across

    def store(b):
        s = lax.rem(b, SLOTS)
        part = (
            pl.ds(pl.multiple_of((b // across) * LANE, LANE), LANE),
            pl.ds(pl.multiple_of(lax.rem(b, across) * load_cols, LANE), load_cols),
        )
        return pltpu.make_async_copy(slot.at[s], out_ref.at[part], sem.at[s])

    @pl.loop(0, blocks)
    def _(b):
        @pl.when(b >= SLOTS)
        def _():
            store(b - SLOTS).wait()

        at_row = pl.ds(pl.multiple_of((b // across) * LANE, LANE), LANE)
        at_col = pl.multiple_of(lax.rem(b, across) * load_cols, LANE)
        for t in range(0, load_cols, STRIP):
            part = slice(t, min(t + STRIP, load_cols))
            here = pl.ds(pl.multiple_of(at_col + t, LANE), part.stop - t)
            product = dot(left[at_row, :], right[:, here])
            x = hi[at_row, here].astype(f32) + lo[at_row, here].astype(f32)
            slot[lax.rem(b, SLOTS), :, part] = x - product
        store(b).start()

    for b in range(max(blocks - SLOTS, 0), blocks):
        store(b).wait()


def best_width(cols, most):
    return max(w for w in range(LANE, most + 1, LANE) if cols % w == 0)


def chunks(cols):
    width = best_width(cols, max(LANE, cols // 7))
    sizes = [width] * (cols // width)
    if width % (2 * LANE) == 0:
        sizes[-1:] = [width // 2] * 2
    ends = [sum(sizes[: k + 1]) for k in range(len(sizes))]
    return [slice(end - size, end) for end, size in zip(ends, sizes)]


def shards(n_row, n_col, gradient, residual, q_init):
    rows, cols = gradient.shape
    parts = chunks(cols)
    load_cols = best_width(cols, 1024)
    n = len(parts)
    vmem = lambda *shape: pltpu.VMEM(shape, f32)
    half = lambda *shape: pltpu.VMEM(shape, bf16)
    dma = pltpu.SemaphoreType.DMA
    anywhere = pl.BlockSpec(memory_space=pl.ANY)
    held = pl.BlockSpec(memory_space=pltpu.VMEM)
    q_factor, hi, lo, left, right = pl.pallas_call(
        functools.partial(kernel, n_row, n_col, parts, load_cols),
        out_shape=(
            jax.ShapeDtypeStruct((4, cols), f32),
            half(rows, cols),
            half(rows, cols),
            half(rows, 32),
            half(32, cols),
        ),
        in_specs=[anywhere, anywhere, held],
        out_specs=(held,) * 5,
        scratch_shapes=[
            half(cols, rows),
            half(cols, rows),
            vmem(SLOTS, LANE, load_cols),
            vmem(SLOTS, LANE, load_cols),
            half(16, cols),
            half(16, rows),
            vmem(16, rows),
            vmem(2, n_col, 4, rows),
            vmem(4, rows),
            vmem(n_row, 4, cols),
            vmem(4, cols),
            vmem(2, n_row, 4, LANE),
            vmem(16, 1, rows),
            dma((SLOTS,)),
            dma((SLOTS,)),
            dma((n_col,)),
            dma((2, n_col)),
            dma((n,)),
            dma((n_row, n)),
            dma((n, n_row)),
            dma((n,)),
            dma((n_row,)),
            dma((2, n_row)),
        ],
        compiler_params=pltpu.CompilerParams(
            collective_id=0, has_side_effects=True, vmem_limit_bytes=35 * 1024 * 1024
        ),
    )(gradient, residual, q_init)
    new_residual = pl.pallas_call(
        functools.partial(subtract, load_cols),
        out_shape=jax.ShapeDtypeStruct((rows, cols), f32),
        in_specs=[held] * 4,
        out_specs=anywhere,
        scratch_shapes=[vmem(SLOTS, LANE, load_cols), dma((SLOTS,))],
        compiler_params=pltpu.CompilerParams(vmem_limit_bytes=4 * 1024 * 1024),
    )(hi, lo, left, right)
    return (q_factor, new_residual)


def solution(mesh):
    in_specs = (P("row", "col"), P("row", "col"), P(None, "col"))
    out_specs = (P(None, "col"), P("row", "col"))
    body = functools.partial(shards, mesh.shape["row"], mesh.shape["col"])
    return jax.shard_map(body, mesh=mesh, in_specs=in_specs, out_specs=out_specs, check_vma=False)
```
